32 devices in a mesh: row: 16 (over z, y, core), col: 2 (over x).
Axes of the slice: x: 2, y: 2, z: 4, core: 2. Of those that a mesh axis runs over, the one named last changes fastest.
Arguments:
- images: bfloat16 [2048, 1024], P(('row', 'col')), as said below
- texts: bfloat16 [2048, 1024], P(('row', 'col')), as said below
- matches: int32 [2048], P('row'), may hold values from 0 to 2047, each once
- logit_scale: float32 [], replicated, may hold values from 20 to 400
Outputs:
- loss: float32 [], replicated
- image_grad: float32 [2048, 1024], P(('row', 'col'))
- text_grad: float32 [2048, 1024], P(('row', 'col'))
The draws below stay inside these ranges and needn't reach their ends.
Inputs may be any that keep to these rules, and one draw needn't show every extreme that they name: `images`: each row is a float embedding whose entries are not all zero. `texts`: each row is a float embedding of order one. `matches`: a permutation of the 2048 text indices.
All inputs are finite; a program needn't handle non-finite values.
Results may differ from the reference program's by a relative error of at most 0.0015.
The reference program's roundings to bfloat16 on the way (of `weights`) count: a program that leaves them out, or rounds other values in their place, can miss the bound.
Values may be sent and summed in bfloat16 or wider, within the bound.
A program may use at most 128 MiB of HBM per device.

```python
import math
import jax
import jax.numpy as jnp
from jax import lax

D = 1024
PAIRS = 2048


def pair_embeddings(key):
    base = jax.random.fold_in(key, 7)
    key_image, key_text = jax.random.split(base, 2)
    images = jax.random.normal(key_image, (PAIRS, D), jnp.float32)
    texts = jax.random.normal(key_text, (PAIRS, D), jnp.float32)
    return (images, texts)


def draw_images(key, part):
    return pair_embeddings(key)[0].astype(jnp.bfloat16)


def draw_texts(key, part):
    return pair_embeddings(key)[1].astype(jnp.bfloat16)


def setup_inputs(seed: int = 0) -> dict:
    key_of = jax.random.split(jax.random.key(seed), 5)
    images = draw_images(jax.random.fold_in(key_of[4], 71), 0)
    texts = draw_texts(jax.random.fold_in(key_of[4], 71), 0)
    matches = jax.random.permutation(key_of[2], PAIRS).astype(jnp.int32)
    logit_scale = jnp.clip(jnp.exp(jax.random.uniform(key_of[3], (), jnp.float32, math.log(20.0), math.log(400.0))), 20.0, 400.0)
    return {"images": images, "texts": texts, "matches": matches, "logit_scale": logit_scale}


EPSILON = 1e-06

def unit_rows(values):
    wide = values.astype(jnp.float32)
    norms = jnp.sqrt(lax.optimization_barrier(jnp.sum(wide * wide, axis=1, keepdims=True)) + EPSILON)
    return (wide / norms, norms)

def back_unit(unit, norms, grad):
    inner = lax.optimization_barrier(jnp.sum(unit * grad, axis=1, keepdims=True))
    return (grad - unit * inner) / norms

def reference(images, texts, matches, logit_scale):
    image_unit, image_norm = unit_rows(images)
    text_unit, text_norm = unit_rows(texts)
    image_low = image_unit.astype(jnp.bfloat16)
    text_low = text_unit.astype(jnp.bfloat16)
    scale = logit_scale.astype(jnp.float32)
    total = images.shape[0]
    block = math.gcd(total, 512)
    count = total // block
    image_blocks = image_low.reshape(count, block, image_low.shape[1])
    match_blocks = matches.reshape(count, block)
    columns = jnp.arange(total, dtype=jnp.int32)

    def forward(carry, item):
        col_max, col_sum, matched = carry
        rows, picks = item
        scores = scale * jnp.dot(rows, text_low.T, preferred_element_type=jnp.float32)
        row_max = lax.optimization_barrier(jnp.max(scores, axis=1))
        row_lse = row_max + jnp.log(lax.optimization_barrier(jnp.sum(jnp.exp(scores - row_max[:, None]), axis=1)))
        top = jnp.maximum(col_max, lax.optimization_barrier(jnp.max(scores, axis=0)))
        col_sum = col_sum * jnp.exp(col_max - top) + lax.optimization_barrier(jnp.sum(jnp.exp(scores - top[None, :]), axis=0))
        mask = picks[:, None] == columns[None, :]
        matched = matched + jnp.sum(jnp.where(mask, scores, jnp.float32(0.0)))
        return ((top, col_sum, matched), row_lse)
    start = (jnp.full((total,), -jnp.inf, jnp.float32), jnp.zeros((total,), jnp.float32), jnp.float32(0.0))
    (col_max, col_sum, matched), row_lse = lax.scan(forward, start, (image_blocks, match_blocks))
    col_lse = col_max + jnp.log(col_sum)
    row_lse = row_lse.reshape(total)
    loss = (jnp.sum(row_lse) + jnp.sum(col_lse)) / (2.0 * total) - matched / total

    def backward(text_acc, item):
        rows, picks, lse_rows = item
        scores = scale * jnp.dot(rows, text_low.T, preferred_element_type=jnp.float32)
        mask = (picks[:, None] == columns[None, :]).astype(jnp.float32)
        weights = 0.5 * jnp.exp(scores - lse_rows[:, None]) + 0.5 * jnp.exp(scores - col_lse[None, :]) - mask
        weights = (scale * weights).astype(jnp.bfloat16)
        image_part = jnp.dot(weights, text_low, preferred_element_type=jnp.float32)
        text_acc = text_acc + lax.dot_general(weights, rows, (((0,), (0,)), ((), ())), preferred_element_type=jnp.float32)
        return (text_acc, image_part)
    text_zero = jnp.zeros(text_low.shape, jnp.float32)
    text_unit_grad, image_parts = lax.scan(backward, text_zero, (image_blocks, match_blocks, row_lse.reshape(count, block)))
    image_unit_grad = image_parts.reshape(total, image_low.shape[1])
    image_grad = back_unit(image_unit, image_norm, image_unit_grad)
    text_grad = back_unit(text_unit, text_norm, text_unit_grad)
    return (loss, image_grad, text_grad)
```

```python
import functools

import jax
import jax.numpy as jnp
from jax import lax
from jax.experimental import pallas as pl
from jax.experimental.pallas import tpu as pltpu
from jax.sharding import PartitionSpec as P

EPSILON = 1e-06
MESH = pl.DeviceIdType.MESH


def merged(value, axis, join):
    pieces = jax.tree.map(lambda part: lax.all_gather(part, axis), value)
    head = jax.tree.map(lambda part: part[0], pieces)
    tail = jax.tree.map(lambda part: part[1:], pieces)
    running, _ = lax.scan(lambda running, piece: (join(running, piece), None), head, tail)
    return running


def unit_rows(values):
    wide = values.astype(jnp.float32)
    norms = jnp.sqrt(jnp.sum(wide * wide, axis=1, keepdims=True) + EPSILON)
    return (wide / norms, norms)


def back_unit(unit, norms, grad):
    inner = jnp.sum(unit * grad, axis=1, keepdims=True)
    return (grad - unit * inner) / norms


def combine_stats(first, second):
    top = jnp.maximum(first[0], second[0])
    return (top, first[1] * jnp.exp(first[0] - top) + second[1] * jnp.exp(second[0] - top))


def on_device(images, texts, matches, logit_scale):
    per_dev = images.shape[0]
    n_row = lax.axis_size("row")
    n_col = lax.axis_size("col")
    total = per_dev * n_row * n_col
    col_pos = lax.axis_index("col")
    row_pos = lax.axis_index("row")
    image_unit, image_norm = unit_rows(images)
    text_unit, text_norm = unit_rows(texts)
    image_low = image_unit.astype(jnp.bfloat16)
    text_low = text_unit.astype(jnp.bfloat16)
    image_rows = lax.all_gather(image_low, "col", axis=0, tiled=True)
    half = 0
    stride = 1
    n_img = image_rows.shape[0]

    def scores_of(piece):
        return logit_scale * lax.dot_general(
            piece, image_rows, (((1,), (1,)), ((), ())), preferred_element_type=jnp.float32
        )

    def match_mask(count):
        place = jnp.arange(count, dtype=jnp.int32)
        owner = place // per_dev * stride + half
        text_ids = owner * (n_col * per_dev) + col_pos * per_dev + place % per_dev
        return text_ids[:, None] == matches[None, :]

    piece = lax.all_gather(text_low, "row", axis=0, tiled=True)
    row_max = jnp.full((n_img,), -jnp.inf, jnp.float32)
    row_sum = jnp.zeros((n_img,), jnp.float32)
    scores = scores_of(piece)
    top = jnp.max(scores, axis=0)
    row_sum = row_sum * jnp.exp(row_max - top) + jnp.sum(jnp.exp(scores - top[None, :]), axis=0)
    piece_max = jnp.max(scores, axis=1)
    piece_sum = jnp.sum(jnp.exp(scores - piece_max[:, None]), axis=1)
    col_max = piece_max
    col_sum = piece_sum
    mask = match_mask(piece.shape[0])
    matched = jnp.sum(jnp.where(mask, scores, jnp.float32(0.0)))
    stats = (top, row_sum, col_max, col_sum, matched)
    row_max, row_sum, col_max, col_sum, matched = stats
    row_max, row_sum = merged((row_max, row_sum), "col", combine_stats)
    slot_max = col_max
    slot_sum = col_sum
    slot_max, slot_sum = merged((slot_max, slot_sum), "row", combine_stats)
    col_max = slot_max
    col_sum = slot_sum
    row_lse = row_max + jnp.log(row_sum)
    col_lse = col_max + jnp.log(col_sum)
    own_rows = jnp.sum(
        lax.dynamic_slice_in_dim(row_lse, (half * n_col + col_pos) * per_dev, per_dev, 0)
    )
    own_cols = jnp.sum(lax.dynamic_slice_in_dim(col_lse, row_pos // stride * per_dev, per_dev, 0))
    share = (own_rows + own_cols) / (2.0 * total) - matched / total
    loss = lax.psum(share, ("row", "col"))
    piece = lax.all_gather(text_low, "row", axis=0, tiled=True)
    count = piece.shape[0]
    scores = scores_of(piece)
    mask = match_mask(count).astype(jnp.float32)
    weights = (
        0.5 * jnp.exp(scores - row_lse[None, :]) + 0.5 * jnp.exp(scores - col_lse[:, None]) - mask
    )
    weights = (logit_scale * weights).astype(jnp.bfloat16)
    image_acc = lax.dot_general(
        weights, piece, (((0,), (0,)), ((), ())), preferred_element_type=jnp.float32
    )
    text_piece = jnp.dot(weights, image_rows, preferred_element_type=jnp.float32)
    text_acc = text_piece
    image_acc, text_acc = (image_acc, text_acc)
    image_unit_grad = lax.psum_scatter(image_acc, "col", scatter_dimension=0, tiled=True)
    text_unit_grad = lax.psum_scatter(text_acc, "row", scatter_dimension=0, tiled=True)
    image_grad = back_unit(image_unit, image_norm, image_unit_grad)
    text_grad = back_unit(text_unit, text_norm, text_unit_grad)
    return (loss, image_grad, text_grad)


def fused_kernel(
    n_row, n_col, img_ref, txt_ref, match_ref, scale_ref, loss_ref, gimg_ref, gtxt_ref,
    raw, low, sc, ex, wbuf, marks, tile, stat, lse, out, qout, qin, sout, sin, part, parts,
    lsem, osem, ssem, rsem,
):
    per = img_ref.shape[0]
    n_dev = n_row * n_col
    total = per * n_dev
    mine = 4 * per
    both = 2 * mine
    row = lax.axis_index("row")
    x = lax.axis_index("col")
    z, y, c = row // 4, (row // 2) % 2, row % 2
    zh, zl = z // 2, z % 2
    scale = scale_ref[0, 0]

    def place(xx, yy, hh, ll, cc):
        return ((hh * 2 + ll) * 4 + yy * 2 + cc, xx)

    def mate(a, k, other=0):
        near, far, cc = k % 2, k // 2, (c + other) % 2
        if a == 0:
            return place((x + near) % 2, y, zh, (zl + far) % 2, cc)
        return place(x, (y + near) % 2, (zh + far) % 2, zl, cc)

    def slot(a, k):
        near, far = k % 2, k // 2
        if a == 0:
            return (zl + far) % 2 * 2 + (x + near) % 2
        return (zh + far) % 2 * 2 + (y + near) % 2

    sibling = mate(0, 0, 1)
    inputs = (img_ref, txt_ref)
    kept = [
        pltpu.make_async_copy(inputs[a], raw.at[a, c * 4 + slot(a, 0)], lsem.at[a])
        for a in range(2)
    ]
    for copy in kept:
        copy.start()
    barrier = pltpu.get_barrier_semaphore()
    greet = [sibling, mate(0, 1), mate(0, 2), mate(0, 3), mate(1, 1), mate(1, 2)]
    for peer in greet:
        pl.semaphore_signal(barrier, inc=1, device_id=peer, device_id_type=MESH)
    marks[c * 2 + zl] = match_ref[...]

    copies = []

    def send(src, dst, target):
        k = len(copies)
        copy = pltpu.make_async_remote_copy(
            src_ref=src, dst_ref=dst, send_sem=ssem.at[k], recv_sem=rsem.at[k],
            device_id=target, device_id_type=MESH,
        )
        copy.start()
        copies.append(copy)
        return copy

    def move(a, k, target):
        ref = raw.at[a, c * 4 + slot(a, k)]
        return send(ref, ref, target)

    def unit_of(a, cc, k):
        piece = cc * 4 + slot(a, k)
        wide = raw[a, piece].astype(jnp.float32)
        norm = jnp.sqrt(jnp.sum(wide * wide, axis=1, keepdims=True) + EPSILON)
        rows = pl.ds(pl.multiple_of(piece * per, per), per)
        low[a, rows, :] = (wide * (1.0 / norm)).astype(jnp.bfloat16)

    pl.semaphore_wait(barrier, len(greet))
    for copy in kept:
        copy.wait()
    got = {}
    got[1, 2] = move(1, 0, mate(1, 2))
    got[0, 1] = move(0, 0, mate(0, 1))
    got[1, 1] = move(1, 0, mate(1, 1))
    got[0, 2] = move(0, 0, mate(0, 2))
    got[0, 3] = move(0, 0, mate(0, 3))
    shared = {(a, 0): move(a, 0, sibling) for a in range(2)}
    ref = match_ref
    mark_far = send(ref, marks.at[c * 2 + zl], mate(0, 2))
    mark_near = send(ref, marks.at[c * 2 + zl], sibling)

    def arrive(a, k):
        got[a, k].wait_recv()
        if (a, k) == (1, 2):
            got[1, 3] = move(1, 2, mate(1, 1))
        shared[a, k] = move(a, k, sibling)

    def from_sibling(a, k):
        shared[a, k].wait_recv()
        unit_of(a, 1 - c, k)

    for a in range(2):
        unit_of(a, c, 0)
    for a in range(2):
        from_sibling(a, 0)
    mark_far.wait_recv()
    far_marks = marks.at[c * 2 + 1 - zl]
    mark_last = send(far_marks, far_marks, sibling)
    arrive(1, 1)
    arrive(0, 1)
    unit_of(1, c, 1)
    arrive(1, 2)
    unit_of(0, c, 1)
    from_sibling(1, 1)
    from_sibling(0, 1)
    unit_of(1, c, 2)
    from_sibling(1, 2)
    arrive(0, 2)
    unit_of(0, c, 2)
    from_sibling(0, 2)
    mark_near.wait_recv()
    mark_last.wait_recv()
    pair = 2 * per
    square = (pair, pair)
    eye = lax.broadcasted_iota(jnp.int32, square, 0) == lax.broadcasted_iota(jnp.int32, square, 1)

    def as_rows(lanes):
        return [
            jnp.sum(
                jnp.where(eye, lanes[:, k * pair : (k + 1) * pair], 0.0), axis=1, keepdims=True
            )
            for k in range(2)
        ]

    def text_ids(shape, dim, base):
        place_ = lax.broadcasted_iota(jnp.int32, shape, dim) + base
        core, unit, item = place_ // mine, place_ // per % 4, place_ % per
        far, near = unit // 2, unit % 2
        return ((((far * 2 + zl) * 4 + near * 2 + core) * 2 + x) * per + item).astype(jnp.float32)

    match_lanes = jnp.concatenate([marks[k].astype(jnp.float32) for k in range(4)], axis=1)
    match_own = jnp.concatenate([marks[c * 2 + k].astype(jnp.float32) for k in range(2)], axis=1)
    match_rows = as_rows(match_own)
    id_lanes = text_ids((1, both), 1, 0)
    id_rows = text_ids((mine, 1), 0, c * mine)
    arrive(0, 3)
    unit_of(0, c, 3)
    arrive(1, 3)
    unit_of(1, c, 3)
    from_sibling(0, 3)
    from_sibling(1, 3)

    own_rows = pl.ds(pl.multiple_of(c * mine, mine), mine)
    news = []
    tops, factor = [None, None], [None, None]
    for a in (1, 0):
        o = 1 - a
        sc[a] = scale * lax.dot_general(
            low[a, own_rows, :], low[o], (((1,), (1,)), ((), ())),
            preferred_element_type=jnp.float32,
        )
        top = jnp.max(sc[a], axis=0, keepdims=True)
        e = jnp.exp(sc[a] - top)
        ex[a] = e
        tops[o] = top
        here = c * 4 + slot(o, 0)
        fields = [top, jnp.sum(e, axis=0, keepdims=True)]
        if o == 0:
            fields.append(
                jnp.sum(jnp.where(id_rows == match_lanes, sc[a], 0.0), axis=0, keepdims=True)
            )
        for k, field in enumerate(fields):
            tile[o, k] = field
            stat[o, here, k] = field
        for k, other in ((3, 1), (3, 0), (2, 1), (2, 0), (1, 1), (1, 0), (0, 1)):
            n = len(fields)
            news.append((o, send(tile.at[o, 0:n], stat.at[o, here, 0:n], mate(o, k, other))))

    lost = []
    for o in (0, 1):
        for owner, copy in news:
            if owner == o:
                copy.wait_recv()
        most = stat[o, 0, 0]
        for k in range(1, 8):
            most = jnp.maximum(most, stat[o, k, 0])
        sums = stat[o, 0, 1] * jnp.exp(stat[o, 0, 0] - most)
        for k in range(1, 8):
            sums = sums + stat[o, k, 1] * jnp.exp(stat[o, k, 0] - most)
        value = most + jnp.log(sums)
        for k in range(2):
            lse[o, k] = value[:, k * mine : (k + 1) * mine]
        factor[o] = 0.5 * jnp.exp(tops[o] - value)
        term = value * (0.5 / total)
        if o == 0:
            hits = stat[0, 0, 2]
            for k in range(1, 8):
                hits = hits + stat[0, k, 2]
            term = term - hits * (1.0 / total)
        lost.append(jnp.sum(term, axis=1, keepdims=True))

    for a in (1, 0):
        o = 1 - a
        columns = as_rows(lse[a, c])
        for k in range(4):
            rows = slice(k * per, (k + 1) * per)
            half = slice(k % 2 * per, (k % 2 + 1) * per)
            value = ex[a, rows, :] * factor[o] + 0.5 * jnp.exp(
                sc[a, rows, :] - columns[k // 2][half]
            )
            if a == 0:
                hit = id_lanes == match_rows[k // 2][half]
            else:
                hit = id_rows[rows] == match_lanes
            value = value - jnp.where(hit, 1.0, 0.0)
            wbuf[a, rows, :] = (scale * value).astype(jnp.bfloat16)

    def grad_of(a, k):
        rows = pl.ds(pl.multiple_of(slot(a, k) * per, per), per)
        return jnp.dot(wbuf[a, rows, :], low[1 - a], preferred_element_type=jnp.float32)

    def pack_send(value, k, target):
        most = jnp.max(jnp.abs(value), axis=0, keepdims=True)
        most = jnp.maximum(most, 1e-30)
        sout[k] = most * (1.0 / 32767.0)
        qout[k] = jnp.round(value * (32767.0 / most)).astype(jnp.int32).astype(jnp.int16)
        return (
            send(qout.at[k], qin.at[k], target),
            send(sout.at[k], sin.at[k], target),
        )

    def unpack(k, pieces):
        for copy in pieces:
            copy.wait_recv()
        return qin[k].astype(jnp.int32).astype(jnp.float32) * sin[k]

    text_diag = pack_send(grad_of(1, 3), 0, mate(1, 1))
    image_diag = pack_send(grad_of(0, 3), 1, mate(0, 3))
    image_far = pack_send(grad_of(0, 2), 2, mate(0, 2))
    image_near = pack_send(grad_of(0, 1), 3, mate(0, 1))
    text_near = pack_send(grad_of(1, 1), 4, mate(1, 1))
    out[1] = grad_of(1, 2)
    text_far = pack_send(out[1] + unpack(0, text_diag), 5, mate(1, 2))

    parts_out = []
    for o in range(2):
        part[o] = jnp.broadcast_to(lost[o], (1, pair))
        parts[o, slot(1 - o, 0)] = part[o]
        for k in (3, 2, 1):
            parts_out.append(
                send(part.at[o], parts.at[o, slot(1 - o, 0)], mate(1 - o, k))
            )

    out[0] = grad_of(0, 0)
    out[1] = grad_of(1, 0)

    def finish(a, k, pieces, last):
        grad = out[a] + unpack(k, pieces)
        if not last:
            out[a] = grad
            return
        wide = raw[a, c * 4 + slot(a, 0)].astype(jnp.float32)
        norm = jnp.sqrt(jnp.sum(wide * wide, axis=1, keepdims=True) + EPSILON)
        inv = 1.0 / norm
        unit = wide * inv
        inner = jnp.sum(unit * grad, axis=1, keepdims=True)
        out[a] = (grad - unit * inner) * inv
        final = pltpu.make_async_copy(out.at[a], (gimg_ref, gtxt_ref)[a], osem.at[a])
        final.start()
        return final

    finish(0, 3, image_near, False)
    finish(1, 4, text_near, False)
    finish(0, 2, image_far, False)
    done = [finish(0, 1, image_diag, True)]
    done.append(finish(1, 5, text_far, True))
    for copy in parts_out:
        copy.wait_recv()
    loss = jnp.zeros((1, 1), jnp.float32)
    for o in range(2):
        for k in range(4):
            loss = loss + parts[o, k][:, 0:1]
    loss_ref[...] = loss
    for copy in copies:
        copy.wait_send()
    for copy in done:
        copy.wait()


def fused(n_row, n_col, images, texts, matches, logit_scale):
    per, d = images.shape
    n_sem = 64
    vmem = pl.BlockSpec(memory_space=pltpu.VMEM)
    anywhere = pl.BlockSpec(memory_space=pl.ANY)
    loss, image_grad, text_grad = pl.pallas_call(
        functools.partial(fused_kernel, n_row, n_col),
        out_shape=(
            jax.ShapeDtypeStruct((1, 1), jnp.float32),
            jax.ShapeDtypeStruct((per, d), jnp.float32),
            jax.ShapeDtypeStruct((per, d), jnp.float32),
        ),
        in_specs=[anywhere, anywhere, vmem, pl.BlockSpec(memory_space=pltpu.SMEM)],
        out_specs=(vmem, anywhere, anywhere),
        scratch_shapes=[
            pltpu.VMEM((2, 8, per, d), jnp.bfloat16),
            pltpu.VMEM((2, 8 * per, d), jnp.bfloat16),
            pltpu.VMEM((2, 4 * per, 8 * per), jnp.float32),
            pltpu.VMEM((2, 4 * per, 8 * per), jnp.float32),
            pltpu.VMEM((2, 4 * per, 8 * per), jnp.bfloat16),
            pltpu.VMEM((4, 1, 2 * per), jnp.int32),
            pltpu.VMEM((2, 3, 1, 8 * per), jnp.float32),
            pltpu.VMEM((2, 8, 3, 1, 8 * per), jnp.float32),
            pltpu.VMEM((2, 2, 1, 4 * per), jnp.float32),
            pltpu.VMEM((2, per, d), jnp.float32),
            pltpu.VMEM((6, per, d), jnp.int16),
            pltpu.VMEM((6, per, d), jnp.int16),
            pltpu.VMEM((6, 1, d), jnp.float32),
            pltpu.VMEM((6, 1, d), jnp.float32),
            pltpu.VMEM((2, 1, 2 * per), jnp.float32),
            pltpu.VMEM((2, 4, 1, 2 * per), jnp.float32),
            pltpu.SemaphoreType.DMA((2,)),
            pltpu.SemaphoreType.DMA((2,)),
            pltpu.SemaphoreType.DMA((n_sem,)),
            pltpu.SemaphoreType.DMA((n_sem,)),
        ],
        compiler_params=pltpu.CompilerParams(
            collective_id=0, has_side_effects=True, vmem_limit_bytes=56 * 1024 * 1024
        ),
    )(images, texts, matches.reshape(1, -1), logit_scale.reshape(1, 1))
    return loss.reshape(()), image_grad, text_grad


def solution(mesh):
    placed = (P(("row", "col"), None), P(("row", "col"), None), P("row"), P())
    n_row, n_col = mesh.shape["row"], mesh.shape["col"]

    def body(images, texts, matches, logit_scale):
        if n_col == 2 and n_row == 16 and matches.shape[0] == 128:
            return fused(n_row, n_col, images, texts, matches, logit_scale)
        return on_device(images, texts, matches, logit_scale)

    return jax.shard_map(
        body,
        mesh=mesh,
        in_specs=placed,
        out_specs=(P(), P(("row", "col"), None), P(("row", "col"), None)),
        check_vma=False,
    )
```

```python
import functools

import jax
import jax.numpy as jnp
from jax import lax
from jax.experimental import pallas as pl
from jax.experimental.pallas import tpu as pltpu
from jax.sharding import PartitionSpec as P

EPSILON = 1e-06
MESH = pl.DeviceIdType.MESH


def merged(value, axis, join):
    pieces = jax.tree.map(lambda part: lax.all_gather(part, axis), value)
    head = jax.tree.map(lambda part: part[0], pieces)
    tail = jax.tree.map(lambda part: part[1:], pieces)
    running, _ = lax.scan(lambda running, piece: (join(running, piece), None), head, tail)
    return running


def unit_rows(values):
    wide = values.astype(jnp.float32)
    norms = jnp.sqrt(jnp.sum(wide * wide, axis=1, keepdims=True) + EPSILON)
    return (wide / norms, norms)


def back_unit(unit, norms, grad):
    inner = jnp.sum(unit * grad, axis=1, keepdims=True)
    return (grad - unit * inner) / norms


def combine_stats(first, second):
    top = jnp.maximum(first[0], second[0])
    return (top, first[1] * jnp.exp(first[0] - top) + second[1] * jnp.exp(second[0] - top))


def on_device(images, texts, matches, logit_scale):
    per_dev = images.shape[0]
    n_row = lax.axis_size("row")
    n_col = lax.axis_size("col")
    total = per_dev * n_row * n_col
    col_pos = lax.axis_index("col")
    row_pos = lax.axis_index("row")
    image_unit, image_norm = unit_rows(images)
    text_unit, text_norm = unit_rows(texts)
    image_low = image_unit.astype(jnp.bfloat16)
    text_low = text_unit.astype(jnp.bfloat16)
    image_rows = lax.all_gather(image_low, "col", axis=0, tiled=True)
    half = 0
    stride = 1
    n_img = image_rows.shape[0]

    def scores_of(piece):
        return logit_scale * lax.dot_general(
            piece, image_rows, (((1,), (1,)), ((), ())), preferred_element_type=jnp.float32
        )

    def match_mask(count):
        place = jnp.arange(count, dtype=jnp.int32)
        owner = place // per_dev * stride + half
        text_ids = owner * (n_col * per_dev) + col_pos * per_dev + place % per_dev
        return text_ids[:, None] == matches[None, :]

    piece = lax.all_gather(text_low, "row", axis=0, tiled=True)
    row_max = jnp.full((n_img,), -jnp.inf, jnp.float32)
    row_sum = jnp.zeros((n_img,), jnp.float32)
    scores = scores_of(piece)
    top = jnp.max(scores, axis=0)
    row_sum = row_sum * jnp.exp(row_max - top) + jnp.sum(jnp.exp(scores - top[None, :]), axis=0)
    piece_max = jnp.max(scores, axis=1)
    piece_sum = jnp.sum(jnp.exp(scores - piece_max[:, None]), axis=1)
    col_max = piece_max
    col_sum = piece_sum
    mask = match_mask(piece.shape[0])
    matched = jnp.sum(jnp.where(mask, scores, jnp.float32(0.0)))
    stats = (top, row_sum, col_max, col_sum, matched)
    row_max, row_sum, col_max, col_sum, matched = stats
    row_max, row_sum = merged((row_max, row_sum), "col", combine_stats)
    slot_max = col_max
    slot_sum = col_sum
    slot_max, slot_sum = merged((slot_max, slot_sum), "row", combine_stats)
    col_max = slot_max
    col_sum = slot_sum
    row_lse = row_max + jnp.log(row_sum)
    col_lse = col_max + jnp.log(col_sum)
    own_rows = jnp.sum(
        lax.dynamic_slice_in_dim(row_lse, (half * n_col + col_pos) * per_dev, per_dev, 0)
    )
    own_cols = jnp.sum(lax.dynamic_slice_in_dim(col_lse, row_pos // stride * per_dev, per_dev, 0))
    share = (own_rows + own_cols) / (2.0 * total) - matched / total
    loss = lax.psum(share, ("row", "col"))
    piece = lax.all_gather(text_low, "row", axis=0, tiled=True)
    count = piece.shape[0]
    scores = scores_of(piece)
    mask = match_mask(count).astype(jnp.float32)
    weights = (
        0.5 * jnp.exp(scores - row_lse[None, :]) + 0.5 * jnp.exp(scores - col_lse[:, None]) - mask
    )
    weights = (logit_scale * weights).astype(jnp.bfloat16)
    image_acc = lax.dot_general(
        weights, piece, (((0,), (0,)), ((), ())), preferred_element_type=jnp.float32
    )
    text_piece = jnp.dot(weights, image_rows, preferred_element_type=jnp.float32)
    text_acc = text_piece
    image_acc, text_acc = (image_acc, text_acc)
    image_unit_grad = lax.psum_scatter(image_acc, "col", scatter_dimension=0, tiled=True)
    text_unit_grad = lax.psum_scatter(text_acc, "row", scatter_dimension=0, tiled=True)
    image_grad = back_unit(image_unit, image_norm, image_unit_grad)
    text_grad = back_unit(text_unit, text_norm, text_unit_grad)
    return (loss, image_grad, text_grad)


def fused_kernel(
    n_row, n_col, img_ref, txt_ref, match_ref, scale_ref, loss_ref, gimg_ref, gtxt_ref,
    raw, low, sc, ex, cols, marks, tile, stat, lse, out, qout, qin, sout, sin, part, parts,
    scalar, lsem, ssem, rsem,
):
    per = img_ref.shape[0]
    n_dev = n_row * n_col
    total = per * n_dev
    mine = 4 * per
    both = 2 * mine
    row = lax.axis_index("row")
    x = lax.axis_index("col")
    z, y, c = row // 4, (row // 2) % 2, row % 2
    zh, zl = z // 2, z % 2

    def place(xx, yy, hh, ll, cc):
        return ((hh * 2 + ll) * 4 + yy * 2 + cc, xx)

    def mate(a, k, other=0):
        near, far, cc = k % 2, k // 2, (c + other) % 2
        if a == 0:
            return place((x + near) % 2, y, zh, (zl + far) % 2, cc)
        return place(x, (y + near) % 2, (zh + far) % 2, zl, cc)

    def slot(a, k):
        near, far = k % 2, k // 2
        if a == 0:
            return (zl + far) % 2 * 2 + (x + near) % 2
        return (zh + far) % 2 * 2 + (y + near) % 2

    chunks, late, halves, near_first = 4, True, 2, False
    sibling = mate(0, 0, 1)
    inputs = (img_ref, txt_ref)
    kept = [
        pltpu.make_async_copy(inputs[1], raw.at[1, c * 4 + slot(1, 0)], lsem.at[1]),
        pltpu.make_async_copy(inputs[0], raw.at[0, c * 4 + slot(0, 0)], lsem.at[0]),
        pltpu.make_async_copy(match_ref, marks.at[c * 2 + zl], lsem.at[2]),
        pltpu.make_async_copy(scale_ref, scalar, lsem.at[3]),
    ]
    for copy in kept:
        copy.start()
    barrier = pltpu.get_barrier_semaphore()
    greet = [sibling, mate(0, 1), mate(0, 2), mate(0, 3), mate(1, 1), mate(1, 2)]
    for peer in greet:
        pl.semaphore_signal(barrier, inc=1, device_id=peer, device_id_type=MESH)

    copies = []

    def send(src, dst, target):
        k = len(copies)
        copy = pltpu.make_async_remote_copy(
            src_ref=src, dst_ref=dst, send_sem=ssem.at[k], recv_sem=rsem.at[k],
            device_id=target, device_id_type=MESH,
        )
        copy.start()
        copies.append(copy)
        return copy

    def move(a, k, target, chunk=None):
        ref = raw.at[a, c * 4 + slot(a, k)]
        if chunk is not None:
            ref = ref.at[pl.ds(chunk * (per // chunks), per // chunks)]
        return send(ref, ref, target)

    def unit_of(a, cc, k):
        piece = cc * 4 + slot(a, k)
        wide = raw[a, piece].astype(jnp.float32)
        norm = jnp.sqrt(jnp.sum(wide * wide, axis=1, keepdims=True) + EPSILON)
        rows = pl.ds(pl.multiple_of(piece * per, per), per)
        low[a, rows, :] = (wide * (1.0 / norm)).astype(jnp.bfloat16)

    with jax.named_scope("enter"):
        pl.semaphore_wait(barrier, len(greet))
    for copy in kept:
        copy.wait()
    scale = scalar[0, 0]
    match_ref = marks.at[c * 2 + zl]
    mark_far = send(match_ref, marks.at[c * 2 + zl], mate(0, 2))
    mark_near = send(match_ref, marks.at[c * 2 + zl], sibling)
    got, shared = {}, {}
    far = [move(1, 0, mate(1, 2), h) for h in range(chunks)]
    got[0, 1] = move(0, 0, mate(0, 1))
    got[1, 1] = move(1, 0, mate(1, 1))
    got[0, 2] = move(0, 0, mate(0, 2))
    if not late:
        got[0, 3] = move(0, 0, mate(0, 3))
    for a in range(2):
        shared[a, 0] = [move(a, 0, sibling)]

    def arrive(a, k):
        with jax.named_scope(f"get{a}{k}"):
            got[a, k].wait_recv()
        shared[a, k] = [move(a, k, sibling)]

    corner = []
    shared[1, 2], shared[1, 3] = [], []

    def relay(h):
        with jax.named_scope(f"far{h}"):
            far[h].wait_recv()
        corner.append(move(1, 2, mate(1, 1), h))
        shared[1, 2].append(move(1, 2, sibling, h))

    def arrive_corner(h):
        with jax.named_scope(f"corner{h}"):
            corner[h].wait_recv()
        shared[1, 3].append(move(1, 3, sibling, h))

    def from_sibling(a, k):
        for copy in shared[a, k]:
            with jax.named_scope(f"share{a}{k}"):
                copy.wait_recv()
        unit_of(a, 1 - c, k)

    for a in range(2):
        unit_of(a, c, 0)
    for a in range(2):
        from_sibling(a, 0)
    arrive(1, 1)
    relay(0)
    if late:
        got[0, 3] = move(0, 0, mate(0, 3))
    arrive(0, 1)
    unit_of(1, c, 1)
    for h in range(1, chunks):
        relay(h)
    unit_of(0, c, 1)
    from_sibling(1, 1)
    from_sibling(0, 1)
    unit_of(1, c, 2)
    with jax.named_scope("mark_far"):
        mark_far.wait_recv()
    far_marks = marks.at[c * 2 + 1 - zl]
    mark_last = send(far_marks, far_marks, sibling)
    from_sibling(1, 2)
    arrive(0, 2)
    unit_of(0, c, 2)
    from_sibling(0, 2)
    mark_near.wait_recv()
    mark_last.wait_recv()
    pair = 2 * per
    square = (pair, pair)
    eye = lax.broadcasted_iota(jnp.int32, square, 0) == lax.broadcasted_iota(jnp.int32, square, 1)

    def as_rows(lanes):
        return [
            jnp.sum(
                jnp.where(eye, lanes[:, k * pair : (k + 1) * pair], 0.0), axis=1, keepdims=True
            )
            for k in range(2)
        ]

    def text_ids(shape, dim, base):
        place_ = lax.broadcasted_iota(jnp.int32, shape, dim) + base
        core, unit, item = place_ // mine, place_ // per % 4, place_ % per
        far, near = unit // 2, unit % 2
        return ((((far * 2 + zl) * 4 + near * 2 + core) * 2 + x) * per + item).astype(jnp.float32)

    match_lanes = jnp.concatenate([marks[k].astype(jnp.float32) for k in range(4)], axis=1)
    match_own = jnp.concatenate([marks[c * 2 + k].astype(jnp.float32) for k in range(2)], axis=1)
    for k, part_rows in enumerate(as_rows(match_own)):
        for h in range(2):
            cols[2, 2 * k + h] = part_rows[h * per : (h + 1) * per]
    id_lanes = text_ids((1, both), 1, 0)
    id_rows = text_ids((mine, 1), 0, c * mine)
    for h in range(chunks - 1):
        arrive_corner(h)
    arrive(0, 3)
    unit_of(0, c, 3)
    arrive_corner(chunks - 1)
    unit_of(1, c, 3)
    from_sibling(0, 3)
    from_sibling(1, 3)

    own_rows = pl.ds(pl.multiple_of(c * mine, mine), mine)
    news = []
    tops, factor = [None, None], [None, None]
    for a in (1, 0):
        o = 1 - a
        sc[a] = scale * lax.dot_general(
            low[a, own_rows, :], low[o], (((1,), (1,)), ((), ())),
            preferred_element_type=jnp.float32,
        )
        top = jnp.max(sc[a], axis=0, keepdims=True)
        e = jnp.exp(sc[a] - top)
        ex[a] = e
        tops[o] = top
        here = c * 4 + slot(o, 0)
        fields = [top, jnp.sum(e, axis=0, keepdims=True)]
        if o == 0:
            fields.append(
                jnp.sum(jnp.where(id_rows == match_lanes, sc[a], 0.0), axis=0, keepdims=True)
            )
        for k, field in enumerate(fields):
            tile[o, k] = field
            stat[o, here, k] = field
        for k, other in ((3, 1), (3, 0), (2, 1), (2, 0), (1, 1), (1, 0), (0, 1)):
            n = len(fields)
            news.append((o, send(tile.at[o, 0:n], stat.at[o, here, 0:n], mate(o, k, other))))

    lost = []
    for o in (0, 1):
        for owner, copy in news:
            if owner == o:
                with jax.named_scope(f"stat{o}"):
                    copy.wait_recv()
        most = stat[o, 0, 0]
        for k in range(1, 8):
            most = jnp.maximum(most, stat[o, k, 0])
        sums = stat[o, 0, 1] * jnp.exp(stat[o, 0, 0] - most)
        for k in range(1, 8):
            sums = sums + stat[o, k, 1] * jnp.exp(stat[o, k, 0] - most)
        value = most + jnp.log(sums)
        for k in range(2):
            lse[o, k] = value[:, k * mine : (k + 1) * mine]
        factor[o] = 0.5 * jnp.exp(tops[o] - value)
        term = value * (0.5 / total)
        if o == 0:
            hits = stat[0, 0, 2]
            for k in range(1, 8):
                hits = hits + stat[0, k, 2]
            term = term - hits * (1.0 / total)
        lost.append(jnp.sum(term, axis=1, keepdims=True))

    for a in (1, 0):
        for k, part_rows in enumerate(as_rows(lse[a, c])):
            for h in range(2):
                cols[a, 2 * k + h] = part_rows[h * per : (h + 1) * per]

    def grad_of(a, k):
        unit = slot(a, k)
        rows = pl.ds(pl.multiple_of(unit * per, per), per)
        value = ex[a, rows, :] * factor[1 - a] + 0.5 * jnp.exp(sc[a, rows, :] - cols[a, unit])
        if a == 0:
            hit = id_lanes == cols[2, unit]
        else:
            hit = text_ids((per, 1), 0, c * mine + unit * per) == match_lanes
        weights = scale * (value - jnp.where(hit, 1.0, 0.0))
        return jnp.dot(
            weights.astype(jnp.bfloat16), low[1 - a], preferred_element_type=jnp.float32
        )

    def pack_send(value, k, target, pieces=1):
        sent = []
        size = per // pieces
        for h in range(pieces):
            block = value[h * size : (h + 1) * size]
            most = jnp.maximum(jnp.max(jnp.abs(block), axis=0, keepdims=True), 1e-30)
            rows = slice(h * size, (h + 1) * size)
            sout[k, h] = most * (1.0 / 32767.0)
            qout[k, rows] = jnp.round(block * (32767.0 / most)).astype(jnp.int32).astype(jnp.int16)
            sent.append(
                (
                    send(qout.at[k, rows], qin.at[k, rows], target),
                    send(sout.at[k, h], sin.at[k, h], target),
                )
            )
        return sent

    def unpack(k, sent, h=0):
        size = per // len(sent)
        for copy in sent[h]:
            with jax.named_scope(f"part{k}"):
                copy.wait_recv()
        rows = slice(h * size, (h + 1) * size)
        return qin[k, rows].astype(jnp.int32).astype(jnp.float32) * sin[k, h]

    text_diag = pack_send(grad_of(1, 3), 0, mate(1, 1), halves)
    if near_first:
        image_near = pack_send(grad_of(0, 1), 3, mate(0, 1))
        image_far = pack_send(grad_of(0, 2), 2, mate(0, 2))
        image_diag = pack_send(grad_of(0, 3), 1, mate(0, 3))
    else:
        image_diag = pack_send(grad_of(0, 3), 1, mate(0, 3))
        image_far = pack_send(grad_of(0, 2), 2, mate(0, 2))
        image_near = pack_send(grad_of(0, 1), 3, mate(0, 1))
    out[1] = grad_of(1, 2)
    text_near = pack_send(grad_of(1, 1), 4, mate(1, 1))
    text_far = []
    size = per // halves
    for h in range(halves):
        rows = slice(h * size, (h + 1) * size)
        block = out[1, rows] + unpack(0, text_diag, h)
        most = jnp.maximum(jnp.max(jnp.abs(block), axis=0, keepdims=True), 1e-30)
        sout[5, h] = most * (1.0 / 32767.0)
        qout[5, rows] = jnp.round(block * (32767.0 / most)).astype(jnp.int32).astype(jnp.int16)
        text_far.append(
            (
                send(qout.at[5, rows], qin.at[5, rows], mate(1, 2)),
                send(sout.at[5, h], sin.at[5, h], mate(1, 2)),
            )
        )

    parts_out = []
    for o in range(2):
        part[o] = jnp.broadcast_to(lost[o], (1, pair))
        parts[o, slot(1 - o, 0)] = part[o]
        for k in (3, 2, 1):
            parts_out.append(
                send(part.at[o], parts.at[o, slot(1 - o, 0)], mate(1 - o, k))
            )

    out[0] = grad_of(0, 0)
    out[1] = grad_of(1, 0)

    def close(a, rows, grad):
        wide = raw[a, c * 4 + slot(a, 0), rows].astype(jnp.float32)
        norm = jnp.sqrt(jnp.sum(wide * wide, axis=1, keepdims=True) + EPSILON)
        inv = 1.0 / norm
        unit = wide * inv
        inner = jnp.sum(unit * grad, axis=1, keepdims=True)
        (gimg_ref, gtxt_ref)[a][rows] = (grad - unit * inner) * inv

    whole = slice(0, per)
    out[0] = out[0] + unpack(3, image_near)
    out[1] = out[1] + unpack(4, text_near)
    out[0] = out[0] + unpack(2, image_far)
    close(0, whole, out[0] + unpack(1, image_diag))
    for h in range(halves):
        rows = slice(h * size, (h + 1) * size)
        close(1, rows, out[1, rows] + unpack(5, text_far, h))
    with jax.named_scope("loss"):
        for copy in parts_out:
            copy.wait_recv()
    loss = jnp.zeros((1, 1), jnp.float32)
    for o in range(2):
        for k in range(4):
            loss = loss + parts[o, k][:, 0:1]
    loss_ref[0, 0] = jnp.sum(loss)
    with jax.named_scope("leave"):
        for copy in copies:
            copy.wait_send()


def fused(n_row, n_col, images, texts, matches, logit_scale):
    per, d = images.shape
    n_sem = 80
    vmem = pl.BlockSpec(memory_space=pltpu.VMEM)
    hbm = pl.BlockSpec(memory_space=pltpu.HBM)
    loss, image_grad, text_grad = pl.pallas_call(
        functools.partial(fused_kernel, n_row, n_col),
        out_shape=(
            pltpu.SMEM((1, 1), jnp.float32),
            pltpu.VMEM((per, d), jnp.float32),
            pltpu.VMEM((per, d), jnp.float32),
        ),
        in_specs=[hbm, hbm, hbm, hbm],
        out_specs=(pl.BlockSpec(memory_space=pltpu.SMEM), vmem, vmem),
        scratch_shapes=[
            pltpu.VMEM((2, 8, per, d), jnp.bfloat16),
            pltpu.VMEM((2, 8 * per, d), jnp.bfloat16),
            pltpu.VMEM((2, 4 * per, 8 * per), jnp.float32),
            pltpu.VMEM((2, 4 * per, 8 * per), jnp.float32),
            pltpu.VMEM((3, 4, per, 1), jnp.float32),
            pltpu.VMEM((4, 1, 2 * per), jnp.int32),
            pltpu.VMEM((2, 3, 1, 8 * per), jnp.float32),
            pltpu.VMEM((2, 8, 3, 1, 8 * per), jnp.float32),
            pltpu.VMEM((2, 2, 1, 4 * per), jnp.float32),
            pltpu.VMEM((2, per, d), jnp.float32),
            pltpu.VMEM((6, per, d), jnp.int16),
            pltpu.VMEM((6, per, d), jnp.int16),
            pltpu.VMEM((6, 2, 1, d), jnp.float32),
            pltpu.VMEM((6, 2, 1, d), jnp.float32),
            pltpu.VMEM((2, 1, 2 * per), jnp.float32),
            pltpu.VMEM((2, 4, 1, 2 * per), jnp.float32),
            pltpu.SMEM((1, 1), jnp.float32),
            pltpu.SemaphoreType.DMA((4,)),
            pltpu.SemaphoreType.DMA((n_sem,)),
            pltpu.SemaphoreType.DMA((n_sem,)),
        ],
        compiler_params=pltpu.CompilerParams(
            collective_id=0, has_side_effects=True, vmem_limit_bytes=56 * 1024 * 1024
        ),
    )(images, texts, matches.reshape(1, -1), logit_scale.reshape(1, 1))
    return loss.reshape(()), image_grad, text_grad


def solution(mesh):
    placed = (P(("row", "col"), None), P(("row", "col"), None), P("row"), P())
    n_row, n_col = mesh.shape["row"], mesh.shape["col"]

    def body(images, texts, matches, logit_scale):
        if n_col == 2 and n_row == 16 and matches.shape[0] == 128:
            return fused(n_row, n_col, images, texts, matches, logit_scale)
        return on_device(images, texts, matches, logit_scale)

    return jax.shard_map(
        body,
        mesh=mesh,
        in_specs=placed,
        out_specs=(P(), P(("row", "col"), None), P(("row", "col"), None)),
        check_vma=False,
    )
```
